32 devices in a mesh: parts: 2 (over y), tm: 4 (over z), sub: 2 (over x), inner: 2 (over core).
Axes of the slice: x: 2, y: 2, z: 4, core: 2. Of those that a mesh axis runs over, the one named last changes fastest.
Arguments:
- guess: float32 [512, 128], P(('parts', 'tm', 'sub', 'inner')), parts along dimension 0, may hold values from -6 to 6
- start: float32 [256], P('parts'), parts along dimension 0, may hold values from -6 to 6
- layer_weight: float32 [256, 64], replicated, may hold values from -0.75 to 0.75
- layer_bias: float32 [256], replicated, may hold values from -4 to 4
- amplitude: float32 [256], replicated, may hold values from 0.5 to 4
Outputs:
- updated: float32 [512, 128], P(('parts', 'tm', 'sub', 'inner')), parts along dimension 0
The draws below stay inside these ranges and needn't reach their ends.
There are 2 independent parts, one for each index of `parts`. The reference program is written for one: setup_inputs(seed, part) draws one part's arguments, and reference() takes and returns one part's arrays. A program takes and returns all parts, laid end to end along the dimension named above; an argument that names none is the same for every part. Nothing has to cross between parts.
All inputs are finite; a program needn't handle non-finite values.
Results may differ from the reference program's by a relative error of at most 0.0003.
Values sent between devices are 32-bit elements; how exact they have to be, the bound alone decides.
No kernel may reach another device: no remote copies, remote signals or barrier semaphores. Data moves between devices by JAX's collectives and lax.ppermute only.
A program may use at most 128 MiB of HBM per device.

```python
import math
import jax
import jax.numpy as jnp
from jax import lax

COORD = 64
HIDDEN_SIZE = 256
STATE = 128
STEPS = 256


def block_levels(key, dims, cuts, low, top_value):
    level, own = 1.0, jax.random.fold_in(key, 6)
    for dim, shards_of in cuts:
        steps = jnp.exp(jax.random.uniform(jax.random.fold_in(own, dim), (shards_of,), jnp.float32, low / len(cuts), top_value / len(cuts)))
        level = level * jnp.repeat(steps, dims[dim] // shards_of).reshape([-1 if axis == dim else 1 for axis in range(len(dims))])
    return level


def gaussian(key, shape, deviation, most, split=(), kind=jnp.bfloat16):
    values = deviation * jax.random.normal(key, shape, jnp.float32)
    if split:
        values = values * block_levels(key, shape, split, -0.22, 0.18)
    return jnp.clip(values, -most, most).astype(kind)


def setup_inputs(seed: int = 0, part: int = 0) -> dict:
    key_of = jax.random.split(jax.random.key(seed), 6)
    part_splits = jax.random.split(jax.random.fold_in(key_of[5], part), 6)
    guess = gaussian(part_splits[0], (STEPS, STATE), 1.0, 6.0, ((0, 16),), jnp.float32)
    start = gaussian(part_splits[1], (STATE,), 1.0, 6.0, (), jnp.float32)
    layer_weight = gaussian(key_of[2], (HIDDEN_SIZE, COORD), COORD ** -0.5, 0.75, (), jnp.float32)
    layer_bias = gaussian(key_of[3], (HIDDEN_SIZE,), 1.0, 4.0, (), jnp.float32)
    amplitude = jnp.clip(jnp.exp(jax.random.uniform(key_of[4], (HIDDEN_SIZE,), jnp.float32, math.log(0.5), math.log(4.0))), 0.5, 4.0)
    return dict(guess=guess, start=start, layer_weight=layer_weight, layer_bias=layer_bias, amplitude=amplitude)


step_size = 0.04
curvature = 0.5


def forces(coords, layer_weight, layer_bias, amplitude):
    hi = lax.Precision.HIGHEST
    pre = jnp.dot(coords, layer_weight.T, precision=hi) + layer_bias
    gate = jax.nn.sigmoid(pre)
    grad = jnp.dot(amplitude * gate, layer_weight, precision=hi) + curvature * coords
    return grad, amplitude * gate * (1.0 - gate)


def hess_apply(vector, layer_weight, weights_d):
    hi = lax.Precision.HIGHEST
    inner_vals = jnp.dot(layer_weight, vector, precision=hi) * weights_d
    return jnp.dot(inner_vals, layer_weight, precision=hi) + curvature * vector


def reference(guess, start, layer_weight, layer_bias, amplitude):
    width = layer_weight.shape[1]
    before = jnp.concatenate([start[None, :], guess[:-1]], axis=0)
    coords, momenta = before[:, :width], before[:, width:]
    grad_zero, curve_zero = forces(coords, layer_weight, layer_bias, amplitude)
    half = momenta - 0.5 * step_size * grad_zero
    moved = coords + step_size * half
    grad_one, curve_one = forces(moved, layer_weight, layer_bias, amplitude)
    landed = half - 0.5 * step_size * grad_one
    image = jnp.concatenate([moved, landed], axis=1)

    def advance(state, items):
        prior, curve_a, curve_b, target = items
        delta = state - prior
        delta_q, delta_p = delta[:width], delta[width:]
        first = hess_apply(delta_q, layer_weight, curve_a)
        new_q = delta_q - 0.5 * step_size * step_size * first + step_size * delta_p
        new_p = delta_p - 0.5 * step_size * first - 0.5 * step_size * hess_apply(new_q, layer_weight, curve_b)
        result = target + jnp.concatenate([new_q, new_p])
        return result, result

    final, states = lax.scan(advance, start, (before, curve_zero, curve_one, image))
    return states
```

```python
import functools
import jax
import jax.numpy as jnp
from jax import lax
from jax.experimental import pallas as pl
from jax.experimental.pallas import tpu as pltpu
from jax.sharding import PartitionSpec as P

step_size = 0.04
curvature = 0.5
PAD = 16

NN = (((1,), (0,)), ((), ()))
NT = (((1,), (1,)), ((), ()))


def split(value):
    high = value.astype(jnp.bfloat16)
    return high, (value - high.astype(jnp.float32)).astype(jnp.bfloat16)


def dot3(left, right, dims=NN):
    (left_high, left_low), (right_high, right_low) = left, right
    one = functools.partial(lax.dot_general, dimension_numbers=dims, preferred_element_type=jnp.float32)
    return one(left_high, right_high) + (one(left_high, right_low) + one(left_low, right_high))


def join(early, late):
    state = late.shape[1]
    product = dot3(split(early), split(late[:state]))
    return jnp.concatenate([product[:state], product[state:] + late[state:]], axis=0)


def local_kernel(guess_ref, start_ref, weight_ref, bias_ref, amp_ref,
                 total_ref, first_ref, tree_ref, kicks_ref, kick_first_ref, shifts_ref, curve_ref):
    rows, state = guess_ref.shape
    width = state // 2
    h = step_size
    guess = guess_ref[...]
    points = jnp.concatenate([guess, jnp.broadcast_to(start_ref[...], (8, state))], axis=0)
    weight = weight_ref[...]
    weight2 = split(weight)
    bias, amp = bias_ref[...], amp_ref[...]
    coords, momenta = points[:, :width], points[:, width:]

    def forces(at):
        gate = jax.nn.sigmoid(dot3(split(at), weight2) + bias)
        scaled = amp * gate
        grad = dot3(split(scaled), weight2, NT) + curvature * at
        return grad, scaled * (1.0 - gate)

    grad_zero, curve_zero = forces(coords)
    half = momenta - 0.5 * h * grad_zero
    moved = coords + h * half
    grad_one, curve_one = forces(moved)
    landed = half - 0.5 * h * grad_one
    image = jnp.concatenate([moved, landed], axis=1)
    first_ref[...] = image[rows:]

    residual = image[:rows - 1] - guess[1:]
    residual = jnp.concatenate([residual, jnp.zeros((1, state), jnp.float32)], axis=0)
    curve_next = jnp.concatenate([curve_zero[1:rows], jnp.zeros((1, curve_zero.shape[1]), jnp.float32)], axis=0)
    pushed = residual[:, :width]
    inner = dot3(split(pushed), weight2) * curve_next
    kicked = 0.5 * h * (dot3(split(inner), weight2, NT) + curvature * pushed)
    shifts = jnp.concatenate([pushed, residual[:, width:] - kicked], axis=1)
    row_id = lax.broadcasted_iota(jnp.int32, (rows, state), 0)
    shifts = jnp.where(row_id == rows - 1, image[:rows], shifts)
    shifts_ref[...] = shifts
    curve_ref[...] = curve_zero[:rows]

    double = jnp.concatenate([weight, weight], axis=0)
    double2 = split(double)
    line = lax.broadcasted_iota(jnp.int32, (width, state), 0)
    lane = lax.broadcasted_iota(jnp.int32, (width, state), 1)
    unit2 = jnp.where((lane == line) | (lane == line + width), 1.0, 0.0)
    right = lane >= width
    unit_top = jnp.where(lane == line, 1.0, 0.0)
    unit_low = jnp.where(lane == line + width, 1.0, 0.0)
    between = (curve_one[:rows] + curve_next) * (0.5 * h)

    def kick(weights_row, count):
        scaled = weight * weights_row
        return dot3(split(scaled), double2, NT) + (0.5 * h * curvature * count) * unit2

    kick_first = kick(curve_zero[0:1] * (0.5 * h), 1)
    kick_first_ref[...] = kick_first
    kicks = [kick(between[j:j + 1], 2 if j < rows - 1 else 1) for j in range(rows)]
    for j in range(0, rows, 2):
        kicks_ref[j // 2] = kicks[j]

    rolled = jnp.concatenate([shifts[:, width:], shifts[:, :width]], axis=1)
    lane_rows = lax.broadcasted_iota(jnp.int32, (rows, state), 1)
    drifted = shifts + jnp.where(lane_rows < width, h * rolled, 0.0)
    level = []
    for k in range(rows // 2):
        a, b = kicks[2 * k], kicks[2 * k + 1]
        moved_row = jnp.broadcast_to(drifted[2 * k:2 * k + 1, :width], (PAD, width))
        left = jnp.concatenate([a[:, :width], moved_row], axis=0)
        both = dot3(split(left), split(b))
        prod = both[:width]
        top = unit_top - jnp.where(right, a + b - h * prod, h * a)
        low = 2 * h * unit_top + unit_low - jnp.where(right, h * a + 2 * h * b - (h * h) * prod, (h * h) * a)
        if k == 0:
            top = top - dot3(split(kick_first[:, :width]), split(low))
        tail = drifted[2 * k:2 * k + 1] - jnp.where(right[:PAD], both[width:], 0.0) + shifts[2 * k + 1:2 * k + 2]
        level.append(jnp.concatenate([top, low, tail], axis=0))
    slot = 0
    while len(level) > 1:
        for item in level[::2]:
            tree_ref[slot] = item
            slot += 1
        level = [join(level[i], level[i + 1]) for i in range(0, len(level), 2)]
    total = level[0]
    total_ref[:state] = total[:state]
    tail_row = lax.broadcasted_iota(jnp.int32, (8, state), 0)
    total_ref[state:] = jnp.where(tail_row == 0, total[state:state + 8], jnp.broadcast_to(guess[0:1], (8, state)))


def spread(packed, state):
    return packed[:state], packed[state:state + 1], packed[state + 1:state + 2]


def apply(state_rows, packed):
    size = packed.shape[1]
    matrix, shift, origin = spread(packed, size)
    return dot3(split(state_rows - origin), split(matrix)) + shift


def compose(early, late):
    size = early.shape[1]
    matrix_a, shift_a, origin_a = spread(early, size)
    matrix_b, shift_b, origin_b = spread(late, size)
    left = jnp.concatenate([matrix_a, jnp.broadcast_to(shift_a - origin_b, (PAD, size))], axis=0)
    product = dot3(split(left), split(matrix_b))
    tail_row = lax.broadcasted_iota(jnp.int32, (8, size), 0)
    tail = jnp.where(tail_row == 0, product[size:size + 8] + shift_b, jnp.broadcast_to(origin_a, (8, size)))
    return jnp.concatenate([product[:size], tail], axis=0)


def ordered(own_ref, others, stack_ref, place, source):
    stack_ref[place] = own_ref[...]
    for index, other in enumerate(others):
        stack_ref[source(place, index + 1)] = other[...]


def total_kernel(source, axis_place, count, own_ref, *refs):
    others, (out_ref, stack_ref) = refs[:count - 1], refs[count - 1:]
    ordered(own_ref, others, stack_ref, axis_place(), source)
    total = stack_ref[0]
    for position in range(1, count):
        total = compose(total, stack_ref[position])
    out_ref[...] = total


def reach_kernel(source, axis_place, count, first_ref, own_ref, *refs):
    others, (out_ref, stack_ref) = refs[:count - 1], refs[count - 1:]
    ordered(own_ref, others, stack_ref, axis_place(), source)
    state = first_ref[...]
    for position in range(count):
        state = apply(state, stack_ref[position])
    out_ref[...] = state


def finish_kernel(groups, rows, entering_ref, guess_ref, weight_ref, tree_ref, kicks_ref, kick_first_ref,
                  shifts_ref, curve_ref, *refs):
    size = guess_ref.shape[1]
    width = size // 2
    h = step_size
    out_ref = refs[-1 - len(groups)]
    stacks = refs[len(refs) - len(groups):]
    state = entering_ref[...]
    used = 0
    for (source, axis_place, count), stack_ref in zip(groups, stacks):
        own_ref, others = refs[used], refs[used + 1:used + count]
        used += count
        place = axis_place()
        ordered(own_ref, others, stack_ref, place, source)
        state = lax.fori_loop(0, place, lambda i, s, stack_ref=stack_ref: apply(s, stack_ref[i]), state)
    guess = guess_ref[...]
    delta = state - guess[0:1]

    def go(vector, item):
        return dot3(split(vector), split(item[:size])) + item[size:size + 8]

    count = rows // 2
    sizes = []
    n = count
    while n > 1:
        sizes.append((n + 1) // 2)
        n //= 2
    starts = [sum(sizes[:i]) for i in range(len(sizes))]
    offsets = {0: delta}
    span = count
    for lev in reversed(range(len(sizes))):
        span //= 2
        for i in range(sizes[lev]):
            offsets[(2 * i + 1) * span] = go(offsets[2 * i * span], tree_ref[starts[lev] + i])

    left = lax.broadcasted_iota(jnp.int32, (8, size), 1) < width

    def kick(vector, matrix):
        moved = dot3(split(vector[:, :width]), split(matrix))
        return vector - jnp.where(left, 0.0, moved)

    def drift(vector):
        other = jnp.concatenate([vector[:, width:], vector[:, :width]], axis=1)
        return vector + jnp.where(left, h * other, 0.0)

    pieces = []
    for i in range(count):
        begin = offsets[i]
        if i > 0:
            pieces.append(begin[0:1])
        else:
            pieces.append(jnp.zeros((1, size), jnp.float32))
            begin = kick(begin, kick_first_ref[...])
        after = kick(drift(begin), kicks_ref[i]) + shifts_ref[2 * i:2 * i + 1]
        pieces.append(after[0:1])
    kicked = jnp.concatenate(pieces, axis=0)
    weight2 = split(weight_ref[...])
    pushed = kicked[:, :width]
    inner = dot3(split(pushed), weight2) * curve_ref[...]
    back = 0.5 * h * (dot3(split(inner), weight2, NT) + curvature * pushed)
    result = kicked + jnp.concatenate([jnp.zeros_like(back), back], axis=1) + guess
    row_id = lax.broadcasted_iota(jnp.int32, (rows, size), 0)
    out_ref[...] = jnp.where(row_id == 0, jnp.broadcast_to(state[0:1], (rows, size)), result)


def call(kernel, out_shape, scratch=(), flops=2_000_000, name=None):
    return pl.pallas_call(
        kernel,
        out_shape=out_shape,
        scratch_shapes=scratch,
        cost_estimate=pl.CostEstimate(flops=flops, bytes_accessed=200_000, transcendentals=0),
        name=name,
    )


def solution(mesh):
    parts, majors, subs, inners = (mesh.shape[name] for name in ("parts", "tm", "sub", "inner"))
    axes = ("tm", "sub", "inner")
    low = 2 if majors % 2 == 0 else 1
    blocks = majors // low
    group = low * subs

    def flat(block, place, inner):
        return (block * group + place) * inners + inner

    def partner(place, turn, count):
        return place ^ turn if count & (count - 1) == 0 else (place + turn) % count

    def origin(place, turn, count):
        return place ^ turn if count & (count - 1) == 0 else lax.rem(place - turn + count, count)

    def inner_place():
        return lax.axis_index("inner")

    def group_place():
        return lax.rem(lax.axis_index("tm"), low) * subs + lax.axis_index("sub")

    def shards(guess, start, layer_weight, layer_bias, amplitude):
        rows, size = guess.shape
        width, hidden = size // 2, layer_weight.shape[0]
        f32 = functools.partial(jax.ShapeDtypeStruct, dtype=jnp.float32)
        packed = f32((size + 8, size))
        weight_t = layer_weight.T
        nodes = rows // 2 - 1
        total, first, tree, kicks, kick_first, shifts, curve = call(
            local_kernel,
            [packed, f32((8, size)), f32((nodes, size + PAD, size)), f32((rows // 2, width, size)),
             f32((width, size)), f32((rows, size)), f32((rows, hidden))],
            name="local_maps", flops=100_000_000,
        )(guess, start[None, :], weight_t, layer_bias[None, :], amplitude[None, :])

        def exchange(value, pairs):
            return lax.ppermute(value, axes, pairs)

        inner_maps = [total]
        for turn in range(1, inners):
            inner_maps.append(exchange(total, [
                (flat(b, g, i), flat(b, g, partner(i, turn, inners)))
                for b in range(blocks) for g in range(group) for i in range(inners)]))
        inner_source = functools.partial(origin, count=inners)
        chip = total
        if inners > 1:
            chip = call(functools.partial(total_kernel, inner_source, inner_place, inners), packed,
                        [pltpu.VMEM((inners,) + packed.shape, jnp.float32)], name="chip_total")(*inner_maps)
        group_maps = [chip]
        for turn in range(1, group):
            group_maps.append(exchange(chip, [
                (flat(b, g, i), flat(b, partner(g, turn, group), (i + 1) % inners))
                for b in range(blocks) for g in range(group) for i in range(inners)]))
        group_source = functools.partial(origin, count=group)
        group_stack = [pltpu.VMEM((group,) + packed.shape, jnp.float32)]

        entering = first
        ahead = []
        if blocks > 1:
            block = lax.axis_index("tm") // low
            top = 1
            while top * 2 < blocks:
                top *= 2
            if blocks > 2:
                span = call(functools.partial(total_kernel, group_source, group_place, group), packed, group_stack,
                            name="block_total")(*group_maps)
            reach = None
            turn = 1
            while turn < top:
                arrived = exchange(span, [
                    (flat(b, g, i), flat((b ^ turn) % blocks if (b ^ turn) < blocks else b, g, (i + 1) % inners))
                    for b in range(blocks) for g in range(group) for i in range(inners)])
                upper = (block & turn) != 0
                known = (block ^ turn) < blocks
                early, late = jnp.where(upper, arrived, span), jnp.where(upper, span, arrived)
                joined = call(lambda a_ref, b_ref, o_ref: o_ref.__setitem__(..., compose(a_ref[...], b_ref[...])),
                              packed, name="span_total")(early, late)
                ahead.append((upper, arrived))
                span = jnp.where(known | upper, joined, span)
                turn *= 2
            if blocks == 2:
                reach = call(functools.partial(reach_kernel, group_source, group_place, group), f32((8, size)),
                             group_stack, name="block_reach")(first, *group_maps)
            else:
                reach = call(lambda f_ref, m_ref, o_ref: o_ref.__setitem__(..., apply(f_ref[...], m_ref[...])),
                             f32((8, size)), name="span_reach")(first, span)
            if blocks == 2 * top:
                pairs = [(flat(b, g, i), flat(b ^ top, g, (i + 1) % inners))
                         for b in range(blocks) for g in range(group) for i in range(inners)]
            else:
                pairs = [(flat(b, g, i), flat((b + top) % blocks, g, (i + 1) % inners))
                         for b in range(blocks) for g in range(group) for i in range(inners)]
            arrived = exchange(reach, pairs)
            entering = jnp.where(block >= top, arrived, first)
            for upper, value in reversed(ahead):
                moved = call(lambda f_ref, m_ref, o_ref: o_ref.__setitem__(..., apply(f_ref[...], m_ref[...])),
                             f32((8, size)), name="span_step")(entering, value)
                entering = jnp.where(upper, moved, entering)

        groups = []
        maps = []
        scratch = []
        if group > 1:
            groups.append((group_source, group_place, group))
            maps += group_maps
            scratch += group_stack
        if inners > 1:
            groups.append((inner_source, inner_place, inners))
            maps += inner_maps
            scratch.append(pltpu.VMEM((inners,) + packed.shape, jnp.float32))
        return call(functools.partial(finish_kernel, groups, rows), f32((rows, size)), scratch, name="finish")(
            entering, guess, weight_t, tree, kicks, kick_first, shifts, curve, *maps)

    placed = (P(("parts",) + axes, None), P("parts"), P(), P(), P())
    return jax.shard_map(
        shards,
        mesh=mesh,
        in_specs=placed,
        out_specs=P(("parts",) + axes, None),
        check_vma=False,
    )
```

```python
import functools
import jax
import jax.numpy as jnp
from jax import lax
from jax.experimental import pallas as pl
from jax.experimental.pallas import tpu as pltpu
from jax.sharding import PartitionSpec as P

step_size = 0.04
curvature = 0.5
PAD = 16

NN = (((1,), (0,)), ((), ()))
NT = (((1,), (1,)), ((), ()))


def split(value):
    high = value.astype(jnp.bfloat16)
    return high, (value - high.astype(jnp.float32)).astype(jnp.bfloat16)


def dot3(left, right, dims=NN):
    (left_high, left_low), (right_high, right_low) = left, right
    one = functools.partial(lax.dot_general, dimension_numbers=dims, preferred_element_type=jnp.float32)
    return one(left_high, right_high) + (one(left_high, right_low) + one(left_low, right_high))


def join(early, late):
    state = late.shape[1]
    product = dot3(split(early), split(late[:state]))
    return jnp.concatenate([product[:state], product[state:] + late[state:]], axis=0)


def local_kernel(guess_in, start_in, weight_in, bias_in, amp_in,
                 total_ref, first_ref, tree_ref, kicks_ref, kick_first_ref, shifts_ref, curve_ref, guess_ref, weight_ref,
                 start_ref, bias_ref, amp_ref, arrived):
    copies = [
        pltpu.make_async_copy(source, target, arrived.at[index])
        for index, (source, target) in enumerate((
            (weight_in, weight_ref), (guess_in, guess_ref), (start_in, start_ref),
            (bias_in, bias_ref), (amp_in, amp_ref)))
    ]
    for copy in copies:
        copy.start()
    for copy in copies:
        copy.wait()
    rows, state = guess_ref.shape
    width = state // 2
    h = step_size
    guess = guess_ref[...]
    points = jnp.concatenate([guess, jnp.broadcast_to(start_ref[...], (8, state))], axis=0)
    weight = weight_ref[...]
    weight2 = split(weight)
    bias, amp = bias_ref[...], amp_ref[...]
    coords, momenta = points[:, :width], points[:, width:]

    def forces(at):
        gate = jax.nn.sigmoid(dot3(split(at), weight2) + bias)
        scaled = amp * gate
        grad = dot3(split(scaled), weight2, NT) + curvature * at
        return grad, scaled * (1.0 - gate)

    grad_zero, curve_zero = forces(coords)
    half = momenta - 0.5 * h * grad_zero
    moved = coords + h * half
    grad_one, curve_one = forces(moved)
    landed = half - 0.5 * h * grad_one
    image = jnp.concatenate([moved, landed], axis=1)
    first_ref[...] = image[rows:]

    residual = image[:rows - 1] - guess[1:]
    residual = jnp.concatenate([residual, jnp.zeros((1, state), jnp.float32)], axis=0)
    curve_next = jnp.concatenate([curve_zero[1:rows], jnp.zeros((1, curve_zero.shape[1]), jnp.float32)], axis=0)
    pushed = residual[:, :width]
    inner = dot3(split(pushed), weight2) * curve_next
    kicked = 0.5 * h * (dot3(split(inner), weight2, NT) + curvature * pushed)
    shifts = jnp.concatenate([pushed, residual[:, width:] - kicked], axis=1)
    row_id = lax.broadcasted_iota(jnp.int32, (rows, state), 0)
    shifts = jnp.where(row_id == rows - 1, image[:rows], shifts)
    shifts_ref[...] = shifts
    curve_ref[...] = curve_zero[:rows]

    double = jnp.concatenate([weight, weight], axis=0)
    double2 = split(double)
    line = lax.broadcasted_iota(jnp.int32, (width, state), 0)
    lane = lax.broadcasted_iota(jnp.int32, (width, state), 1)
    unit2 = jnp.where((lane == line) | (lane == line + width), 1.0, 0.0)
    right = lane >= width
    unit_top = jnp.where(lane == line, 1.0, 0.0)
    unit_low = jnp.where(lane == line + width, 1.0, 0.0)
    between = (curve_one[:rows] + curve_next) * (0.5 * h)

    def kick(weights_row, count):
        scaled = weight * weights_row
        return dot3(split(scaled), double2, NT) + (0.5 * h * curvature * count) * unit2

    kick_first = kick(curve_zero[0:1] * (0.5 * h), 1)
    kick_first_ref[...] = kick_first
    kicks = [kick(between[j:j + 1], 2 if j < rows - 1 else 1) for j in range(rows)]
    for j in range(0, rows, 2):
        kicks_ref[j // 2] = kicks[j]

    rolled = jnp.concatenate([shifts[:, width:], shifts[:, :width]], axis=1)
    lane_rows = lax.broadcasted_iota(jnp.int32, (rows, state), 1)
    drifted = shifts + jnp.where(lane_rows < width, h * rolled, 0.0)
    level = []
    for k in range(rows // 2):
        a, b = kicks[2 * k], kicks[2 * k + 1]
        moved_row = jnp.broadcast_to(drifted[2 * k:2 * k + 1, :width], (PAD, width))
        left = jnp.concatenate([a[:, :width], moved_row], axis=0)
        both = dot3(split(left), split(b))
        prod = both[:width]
        top = unit_top - jnp.where(right, a + b - h * prod, h * a)
        low = 2 * h * unit_top + unit_low - jnp.where(right, h * a + 2 * h * b - (h * h) * prod, (h * h) * a)
        if k == 0:
            top = top - dot3(split(kick_first[:, :width]), split(low))
        tail = drifted[2 * k:2 * k + 1] - jnp.where(right[:PAD], both[width:], 0.0) + shifts[2 * k + 1:2 * k + 2]
        level.append(jnp.concatenate([top, low, tail], axis=0))
    slot = 0
    while len(level) > 1:
        for item in level[::2]:
            tree_ref[slot] = item
            slot += 1
        level = [join(level[i], level[i + 1]) for i in range(0, len(level), 2)]
    total = level[0]
    total_ref[:state] = total[:state]
    tail_row = lax.broadcasted_iota(jnp.int32, (8, state), 0)
    total_ref[state:] = jnp.where(tail_row == 0, total[state:state + 8], jnp.broadcast_to(guess[0:1], (8, state)))


def spread(packed, state):
    return packed[:state], packed[state:state + 1], packed[state + 1:state + 2]


def apply(state_rows, packed):
    size = packed.shape[1]
    matrix, shift, origin = spread(packed, size)
    return dot3(split(state_rows - origin), split(matrix)) + shift


def compose(early, late):
    size = early.shape[1]
    matrix_a, shift_a, origin_a = spread(early, size)
    matrix_b, shift_b, origin_b = spread(late, size)
    left = jnp.concatenate([matrix_a, jnp.broadcast_to(shift_a - origin_b, (PAD, size))], axis=0)
    product = dot3(split(left), split(matrix_b))
    tail_row = lax.broadcasted_iota(jnp.int32, (8, size), 0)
    tail = jnp.where(tail_row == 0, product[size:size + 8] + shift_b, jnp.broadcast_to(origin_a, (8, size)))
    return jnp.concatenate([product[:size], tail], axis=0)


def ordered(own_ref, others, stack_ref, place, source):
    stack_ref[place] = own_ref[...]
    for index, other in enumerate(others):
        stack_ref[source(place, index + 1)] = other[...]


def total_kernel(source, axis_place, count, own_ref, *refs):
    others, (out_ref, stack_ref) = refs[:count - 1], refs[count - 1:]
    ordered(own_ref, others, stack_ref, axis_place(), source)
    total = stack_ref[0]
    for position in range(1, count):
        total = compose(total, stack_ref[position])
    out_ref[...] = total


def reach_kernel(source, axis_place, count, first_ref, own_ref, *refs):
    others, (out_ref, stack_ref) = refs[:count - 1], refs[count - 1:]
    ordered(own_ref, others, stack_ref, axis_place(), source)
    state = first_ref[...]
    for position in range(count):
        state = apply(state, stack_ref[position])
    out_ref[...] = state


def finish_kernel(groups, rows, entering_ref, guess_ref, weight_ref, tree_ref, kicks_ref, kick_first_ref,
                  shifts_ref, curve_ref, *refs):
    size = guess_ref.shape[1]
    width = size // 2
    h = step_size
    out_ref = refs[-1 - len(groups)]
    stacks = refs[len(refs) - len(groups):]
    state = entering_ref[...]
    used = 0
    for (source, axis_place, count), stack_ref in zip(groups, stacks):
        own_ref, others = refs[used], refs[used + 1:used + count]
        used += count
        place = axis_place()
        ordered(own_ref, others, stack_ref, place, source)
        state = lax.fori_loop(0, place, lambda i, s, stack_ref=stack_ref: apply(s, stack_ref[i]), state)
    guess = guess_ref[...]
    delta = state - guess[0:1]

    def go(vector, item):
        return dot3(split(vector), split(item[:size])) + item[size:size + 8]

    count = rows // 2
    sizes = []
    n = count
    while n > 1:
        sizes.append((n + 1) // 2)
        n //= 2
    starts = [sum(sizes[:i]) for i in range(len(sizes))]
    offsets = {0: delta}
    span = count
    for lev in reversed(range(len(sizes))):
        span //= 2
        for i in range(sizes[lev]):
            offsets[(2 * i + 1) * span] = go(offsets[2 * i * span], tree_ref[starts[lev] + i])

    left = lax.broadcasted_iota(jnp.int32, (8, size), 1) < width

    def kick(vector, matrix):
        moved = dot3(split(vector[:, :width]), split(matrix))
        return vector - jnp.where(left, 0.0, moved)

    def drift(vector):
        other = jnp.concatenate([vector[:, width:], vector[:, :width]], axis=1)
        return vector + jnp.where(left, h * other, 0.0)

    pieces = []
    for i in range(count):
        begin = offsets[i]
        if i > 0:
            pieces.append(begin[0:1])
        else:
            pieces.append(jnp.zeros((1, size), jnp.float32))
            begin = kick(begin, kick_first_ref[...])
        after = kick(drift(begin), kicks_ref[i]) + shifts_ref[2 * i:2 * i + 1]
        pieces.append(after[0:1])
    kicked = jnp.concatenate(pieces, axis=0)
    weight2 = split(weight_ref[...])
    pushed = kicked[:, :width]
    inner = dot3(split(pushed), weight2) * curve_ref[...]
    back = 0.5 * h * (dot3(split(inner), weight2, NT) + curvature * pushed)
    result = kicked + jnp.concatenate([jnp.zeros_like(back), back], axis=1) + guess
    row_id = lax.broadcasted_iota(jnp.int32, (rows, size), 0)
    out_ref[...] = jnp.where(row_id == 0, jnp.broadcast_to(state[0:1], (rows, size)), result)


def call(kernel, out_shape, scratch=(), flops=2_000_000, name=None, **specs):
    return pl.pallas_call(
        kernel,
        **specs,
        out_shape=out_shape,
        scratch_shapes=scratch,
        compiler_params=pltpu.CompilerParams(vmem_limit_bytes=8 << 20),
        cost_estimate=pl.CostEstimate(flops=flops, bytes_accessed=200_000, transcendentals=0),
        name=name,
    )


def solution(mesh):
    parts, majors, subs, inners = (mesh.shape[name] for name in ("parts", "tm", "sub", "inner"))
    axes = ("tm", "sub", "inner")
    low = 2 if majors % 2 == 0 else 1
    blocks = majors // low
    group = low * subs

    def flat(block, place, inner):
        return (block * group + place) * inners + inner

    def partner(place, turn, count):
        return place ^ turn if count & (count - 1) == 0 else (place + turn) % count

    def origin(place, turn, count):
        return place ^ turn if count & (count - 1) == 0 else lax.rem(place - turn + count, count)

    def inner_place():
        return lax.axis_index("inner")

    def group_place():
        return lax.rem(lax.axis_index("tm"), low) * subs + lax.axis_index("sub")

    def shards(guess, start, layer_weight, layer_bias, amplitude):
        rows, size = guess.shape
        width, hidden = size // 2, layer_weight.shape[0]
        f32 = functools.partial(jax.ShapeDtypeStruct, dtype=jnp.float32)
        packed = f32((size + 8, size))
        weight_t = layer_weight.T
        nodes = rows // 2 - 1
        total, first, tree, kicks, kick_first, shifts, curve, guess, weight_t = call(
            local_kernel,
            [packed, f32((8, size)), f32((nodes, size + PAD, size)), f32((rows // 2, width, size)),
             f32((width, size)), f32((rows, size)), f32((rows, hidden)), f32((rows, size)), f32((width, hidden))],
            [pltpu.VMEM((1, size), jnp.float32), pltpu.VMEM((1, hidden), jnp.float32), pltpu.VMEM((1, hidden), jnp.float32),
             pltpu.SemaphoreType.DMA((5,))],
            name="local_maps", flops=100_000_000, in_specs=[pl.BlockSpec(memory_space=pltpu.HBM)] * 5,
        )(*(pltpu.with_memory_space_constraint(value, pltpu.HBM) for value in (
            guess, start[None, :], weight_t, layer_bias[None, :], amplitude[None, :])))

        def exchange(value, pairs):
            return lax.ppermute(value, axes, pairs)

        inner_maps = [total]
        for turn in range(1, inners):
            inner_maps.append(exchange(total, [
                (flat(b, g, i), flat(b, g, partner(i, turn, inners)))
                for b in range(blocks) for g in range(group) for i in range(inners)]))
        inner_source = functools.partial(origin, count=inners)
        chip = total
        if inners > 1:
            chip = call(functools.partial(total_kernel, inner_source, inner_place, inners), packed,
                        [pltpu.VMEM((inners,) + packed.shape, jnp.float32)], name="chip_total")(*inner_maps)
        group_maps = [chip]
        for turn in range(1, group):
            group_maps.append(exchange(chip, [
                (flat(b, g, i), flat(b, partner(g, turn, group), (i + 1) % inners))
                for b in range(blocks) for g in range(group) for i in range(inners)]))
        group_source = functools.partial(origin, count=group)
        group_stack = [pltpu.VMEM((group,) + packed.shape, jnp.float32)]

        entering = first
        ahead = []
        if blocks > 1:
            block = lax.axis_index("tm") // low
            top = 1
            while top * 2 < blocks:
                top *= 2
            if blocks > 2:
                span = call(functools.partial(total_kernel, group_source, group_place, group), packed, group_stack,
                            name="block_total")(*group_maps)
            reach = None
            turn = 1
            while turn < top:
                arrived = exchange(span, [
                    (flat(b, g, i), flat((b ^ turn) % blocks if (b ^ turn) < blocks else b, g, (i + 1) % inners))
                    for b in range(blocks) for g in range(group) for i in range(inners)])
                upper = (block & turn) != 0
                known = (block ^ turn) < blocks
                early, late = jnp.where(upper, arrived, span), jnp.where(upper, span, arrived)
                joined = call(lambda a_ref, b_ref, o_ref: o_ref.__setitem__(..., compose(a_ref[...], b_ref[...])),
                              packed, name="span_total")(early, late)
                ahead.append((upper, arrived))
                span = jnp.where(known | upper, joined, span)
                turn *= 2
            if blocks == 2:
                reach = call(functools.partial(reach_kernel, group_source, group_place, group), f32((8, size)),
                             group_stack, name="block_reach")(first, *group_maps)
            else:
                reach = call(lambda f_ref, m_ref, o_ref: o_ref.__setitem__(..., apply(f_ref[...], m_ref[...])),
                             f32((8, size)), name="span_reach")(first, span)
            if blocks == 2 * top:
                pairs = [(flat(b, g, i), flat(b ^ top, g, (i + 1) % inners))
                         for b in range(blocks) for g in range(group) for i in range(inners)]
            else:
                pairs = [(flat(b, g, i), flat((b + top) % blocks, g, (i + 1) % inners))
                         for b in range(blocks) for g in range(group) for i in range(inners)]
            arrived = exchange(reach, pairs)
            entering = jnp.where(block >= top, arrived, first)
            for upper, value in reversed(ahead):
                moved = call(lambda f_ref, m_ref, o_ref: o_ref.__setitem__(..., apply(f_ref[...], m_ref[...])),
                             f32((8, size)), name="span_step")(entering, value)
                entering = jnp.where(upper, moved, entering)

        groups = []
        maps = []
        scratch = []
        if group > 1:
            groups.append((group_source, group_place, group))
            maps += group_maps
            scratch += group_stack
        if inners > 1:
            groups.append((inner_source, inner_place, inners))
            maps += inner_maps
            scratch.append(pltpu.VMEM((inners,) + packed.shape, jnp.float32))
        return call(functools.partial(finish_kernel, groups, rows), f32((rows, size)), scratch, name="finish")(
            entering, guess, weight_t, tree, kicks, kick_first, shifts, curve, *maps)

    placed = (P(("parts",) + axes, None), P("parts"), P(), P(), P())
    return jax.shard_map(
        shards,
        mesh=mesh,
        in_specs=placed,
        out_specs=P(("parts",) + axes, None),
        check_vma=False,
    )
```

```python
import functools
import jax
import jax.numpy as jnp
from jax import lax
from jax.experimental import pallas as pl
from jax.experimental.pallas import tpu as pltpu
from jax.sharding import PartitionSpec as P

step_size = 0.04
curvature = 0.5
PAD = 16

NN = (((1,), (0,)), ((), ()))
NT = (((1,), (1,)), ((), ()))


def split(value):
    high = value.astype(jnp.bfloat16)
    return high, (value - high.astype(jnp.float32)).astype(jnp.bfloat16)


def dot3(left, right, dims=NN):
    (left_high, left_low), (right_high, right_low) = left, right
    one = functools.partial(lax.dot_general, dimension_numbers=dims, preferred_element_type=jnp.float32)
    return one(left_high, right_high) + (one(left_high, right_low) + one(left_low, right_high))


def dot3w(left, right):
    (left_high, left_low), (right_high, right_low) = left, right
    size = right_high.shape[1]
    both = jnp.dot(left_high, jnp.concatenate([right_high, right_low], axis=1), preferred_element_type=jnp.float32)
    return both[:, :size] + (both[:, size:] + jnp.dot(left_low, right_high, preferred_element_type=jnp.float32))


def join(early, late):
    state = late.shape[1]
    product = dot3w(split(early), split(late[:state]))
    return jnp.concatenate([product[:state], product[state:] + late[state:]], axis=0)


def local_kernel(guess_in, start_in, weight_in, bias_in, amp_in,
                 total_ref, first_ref, tree_ref, kicks_ref, kick_first_ref, shifts_ref, curve_ref, guess_ref, weight_ref,
                 start_ref, bias_ref, amp_ref, high_ref, low_ref, arrived):
    copies = [
        pltpu.make_async_copy(source, target, arrived.at[index])
        for index, (source, target) in enumerate((
            (weight_in, weight_ref), (guess_in, guess_ref), (start_in, start_ref),
            (bias_in, bias_ref), (amp_in, amp_ref)))
    ]
    for copy in copies:
        copy.start()
    for copy in copies:
        copy.wait()
    rows, state = guess_ref.shape
    width = state // 2
    h = step_size
    guess = guess_ref[...]
    points = jnp.concatenate([guess, jnp.broadcast_to(start_ref[...], (8, state))], axis=0)
    weight = weight_ref[...]
    weight2 = split(weight)
    bias, amp = bias_ref[...], amp_ref[...]
    coords, momenta = points[:, :width], points[:, width:]

    def forces(at):
        gate = jax.nn.sigmoid(dot3(split(at), weight2) + bias)
        scaled = amp * gate
        grad = dot3(split(scaled), weight2, NT) + curvature * at
        return grad, scaled * (1.0 - gate)

    grad_zero, curve_zero = forces(coords)
    half = momenta - 0.5 * h * grad_zero
    moved = coords + h * half
    grad_one, curve_one = forces(moved)
    landed = half - 0.5 * h * grad_one
    image = jnp.concatenate([moved, landed], axis=1)
    first_ref[...] = image[rows:]

    residual = image[:rows - 1] - guess[1:]
    residual = jnp.concatenate([residual, jnp.zeros((1, state), jnp.float32)], axis=0)
    curve_next = jnp.concatenate([curve_zero[1:rows], jnp.zeros((1, curve_zero.shape[1]), jnp.float32)], axis=0)
    pushed = residual[:, :width]
    inner = dot3(split(pushed), weight2) * curve_next
    kicked = 0.5 * h * (dot3(split(inner), weight2, NT) + curvature * pushed)
    shifts = jnp.concatenate([pushed, residual[:, width:] - kicked], axis=1)
    row_id = lax.broadcasted_iota(jnp.int32, (rows, state), 0)
    shifts = jnp.where(row_id == rows - 1, image[:rows], shifts)
    shifts_ref[...] = shifts
    curve_ref[...] = curve_zero[:rows]

    double = jnp.concatenate([weight, weight], axis=0)
    double2 = split(double)
    line = lax.broadcasted_iota(jnp.int32, (width, state), 0)
    lane = lax.broadcasted_iota(jnp.int32, (width, state), 1)
    unit2 = jnp.where((lane == line) | (lane == line + width), 1.0, 0.0)
    right = lane >= width
    unit_top = jnp.where(lane == line, 1.0, 0.0)
    unit_low = jnp.where(lane == line + width, 1.0, 0.0)
    between = (curve_one[:rows] + curve_next) * (0.5 * h)

    rows_of_kick = [curve_zero[0:1] * (0.5 * h)] + [between[j:j + 1] for j in range(rows)]
    for j, weights_row in enumerate(rows_of_kick):
        scaled_high, scaled_low = split(weight * weights_row)
        high_ref[j * width:(j + 1) * width] = scaled_high
        low_ref[j * width:(j + 1) * width] = scaled_low
    product = lax.dot_general(high_ref[...], jnp.concatenate(double2, axis=0), NT, preferred_element_type=jnp.float32)
    small = lax.dot_general(low_ref[...], double2[0], NT, preferred_element_type=jnp.float32)
    product = product[:, :state] + (product[:, state:] + small)
    kicks = [
        product[j * width:(j + 1) * width] + (0.5 * h * curvature * (1 if j in (0, rows) else 2)) * unit2
        for j in range(rows + 1)
    ]
    kick_first, kicks = kicks[0], kicks[1:]
    kick_first_ref[...] = kick_first
    for j in range(0, rows, 2):
        kicks_ref[j // 2] = kicks[j]

    rolled = jnp.concatenate([shifts[:, width:], shifts[:, :width]], axis=1)
    lane_rows = lax.broadcasted_iota(jnp.int32, (rows, state), 1)
    drifted = shifts + jnp.where(lane_rows < width, h * rolled, 0.0)
    level = []
    for k in range(rows // 2):
        a, b = kicks[2 * k], kicks[2 * k + 1]
        moved_row = jnp.broadcast_to(drifted[2 * k:2 * k + 1, :width], (PAD, width))
        left = jnp.concatenate([a[:, :width], moved_row], axis=0)
        both = dot3(split(left), split(b))
        prod = both[:width]
        top = unit_top - jnp.where(right, a + b - h * prod, h * a)
        low = 2 * h * unit_top + unit_low - jnp.where(right, h * a + 2 * h * b - (h * h) * prod, (h * h) * a)
        if k == 0:
            top = top - dot3(split(kick_first[:, :width]), split(low))
        tail = drifted[2 * k:2 * k + 1] - jnp.where(right[:PAD], both[width:], 0.0) + shifts[2 * k + 1:2 * k + 2]
        level.append(jnp.concatenate([top, low, tail], axis=0))
    slot = 0
    while len(level) > 1:
        for item in level[::2]:
            tree_ref[slot] = item
            slot += 1
        level = [join(level[i], level[i + 1]) for i in range(0, len(level), 2)]
    total = level[0]
    total_ref[:state] = total[:state]
    tail_row = lax.broadcasted_iota(jnp.int32, (8, state), 0)
    total_ref[state:] = jnp.where(tail_row == 0, total[state:state + 8], jnp.broadcast_to(guess[0:1], (8, state)))


def spread(packed, state):
    return packed[:state], packed[state:state + 1], packed[state + 1:state + 2]


def apply(state_rows, packed):
    size = packed.shape[1]
    matrix, shift, origin = spread(packed, size)
    return dot3(split(state_rows - origin), split(matrix)) + shift


def compose(early, late):
    size = early.shape[1]
    matrix_a, shift_a, origin_a = spread(early, size)
    matrix_b, shift_b, origin_b = spread(late, size)
    left = jnp.concatenate([matrix_a, jnp.broadcast_to(shift_a - origin_b, (PAD, size))], axis=0)
    product = dot3(split(left), split(matrix_b))
    tail_row = lax.broadcasted_iota(jnp.int32, (8, size), 0)
    tail = jnp.where(tail_row == 0, product[size:size + 8] + shift_b, jnp.broadcast_to(origin_a, (8, size)))
    return jnp.concatenate([product[:size], tail], axis=0)


def ordered(own_ref, others, stack_ref, place, source):
    stack_ref[place] = own_ref[...]
    for index, other in enumerate(others):
        stack_ref[source(place, index + 1)] = other[...]


def total_kernel(source, axis_place, count, own_ref, *refs):
    others, (out_ref, stack_ref) = refs[:count - 1], refs[count - 1:]
    ordered(own_ref, others, stack_ref, axis_place(), source)
    total = stack_ref[0]
    for position in range(1, count):
        total = compose(total, stack_ref[position])
    out_ref[...] = total


def reach_kernel(source, axis_place, count, first_ref, own_ref, *refs):
    others, (out_ref, stack_ref) = refs[:count - 1], refs[count - 1:]
    ordered(own_ref, others, stack_ref, axis_place(), source)
    state = first_ref[...]
    for position in range(count):
        state = apply(state, stack_ref[position])
    out_ref[...] = state


def prefix_kernel(tree_ref, kicks_ref, kick_first_ref, shifts_ref, curve_ref, guess_ref, weight_ref,
                  maps_ref, offsets_ref, high_ref, low_ref):
    rows, size = guess_ref.shape
    width = size // 2
    h = step_size
    weight = weight_ref[...]
    double2 = split(jnp.concatenate([weight, weight], axis=0))
    for j in range(1, rows):
        scaled_high, scaled_low = split(weight * (curve_ref[j:j + 1] * (0.5 * h)))
        high_ref[(j - 1) * width:j * width] = scaled_high
        low_ref[(j - 1) * width:j * width] = scaled_low
    product = lax.dot_general(high_ref[...], jnp.concatenate(double2, axis=0), NT, preferred_element_type=jnp.float32)
    small = lax.dot_general(low_ref[...], double2[0], NT, preferred_element_type=jnp.float32)
    product = product[:, :size] + (product[:, size:] + small)
    line = lax.broadcasted_iota(jnp.int32, (width, size), 0)
    lane = lax.broadcasted_iota(jnp.int32, (width, size), 1)
    unit2 = jnp.where((lane == line) | (lane == line + width), 0.5 * h * curvature, 0.0)
    whole_line = lax.broadcasted_iota(jnp.int32, (size + PAD, size), 0)
    whole_lane = lax.broadcasted_iota(jnp.int32, (size + PAD, size), 1)
    left = whole_lane < width
    unit = jnp.where(whole_line == whole_lane, 1.0, 0.0)

    def kick(item, matrix):
        return item - jnp.where(left, 0.0, dot3w(split(item[:, :width]), split(matrix)))

    def drift(item):
        other = jnp.concatenate([item[:, width:], item[:, :width]], axis=1)
        return item + jnp.where(left, h * other, 0.0)

    count = rows // 2
    starts, sizes, n = [0], [], count
    while n > 1:
        sizes.append(n // 2)
        starts.append(starts[-1] + n // 2)
        n //= 2
    kicked = {0: kick(unit, kick_first_ref[...])}
    for k in range(1, count):
        low = k & -k
        node = tree_ref[starts[low.bit_length() - 1] + (k - low) // low // 2]
        kicked[2 * k] = node if k == low else join(kicked[2 * (k - low)], node)
    maps_ref[0] = unit[:size]
    offsets_ref[0:1] = guess_ref[0:1]
    for k in range(count):
        after = kick(drift(kicked[2 * k]), kicks_ref[k])
        tail = after[size:] + shifts_ref[2 * k:2 * k + 1]
        kicked[2 * k + 1] = jnp.concatenate([after[:size], tail], axis=0)
    for t in range(1, rows):
        item = kick(kicked[t], -(product[(t - 1) * width:t * width] + unit2))
        maps_ref[t] = item[:size]
        offsets_ref[t:t + 1] = item[size:size + 1] + guess_ref[t:t + 1]


def ahead_kernel(groups, guess_ref, *refs):
    size = guess_ref.shape[1]
    out_ref, shift_ref, origin_ref = refs[-3 - len(groups):len(refs) - len(groups)]
    stacks = refs[len(refs) - len(groups):]
    line = lax.broadcasted_iota(jnp.int32, (size + 8, size), 0)
    lane = lax.broadcasted_iota(jnp.int32, (size + 8, size), 1)
    total = jnp.where(line == lane, 1.0, 0.0)
    empty = True
    used = 0
    for (source, axis_place, count), stack_ref in zip(groups, stacks):
        own_ref, others = refs[used], refs[used + 1:used + count]
        used += count
        place = axis_place()
        ordered(own_ref, others, stack_ref, place, source)

        def body(i, carry, stack_ref=stack_ref):
            return compose(carry, stack_ref[i])

        if empty is True:
            total = lax.fori_loop(1, place, body, jnp.where(place > 0, stack_ref[0], total))
            empty = place == 0
        else:
            first = jnp.where(empty, stack_ref[0], compose(total, stack_ref[0]))
            total = lax.fori_loop(1, place, body, jnp.where(place > 0, first, total))
            empty = empty & (place == 0)
    out_ref[...] = total[:size].T
    shift = total[size:size + 1] - guess_ref[0:1]
    shift_ref[...] = jnp.broadcast_to(shift, (size, size)).T
    origin_ref[...] = jnp.broadcast_to(total[size + 1:size + 2], (8, size))


def finish_kernel(later_block, arrived_ref, first_ref, ahead_ref, shift_ref, origin_ref, maps_ref, offsets_ref, out_ref):
    rows, size = offsets_ref.shape
    state = jnp.where(later_block(), arrived_ref[0:1], first_ref[0:1]) - origin_ref[0:1]
    delta = jnp.sum(ahead_ref[...] * state, axis=1, keepdims=True) + shift_ref[...]
    pieces = [jnp.sum(maps_ref[t] * delta, axis=0, keepdims=True) for t in range(rows)]
    out_ref[...] = jnp.concatenate(pieces, axis=0) + offsets_ref[...]


def call(kernel, out_shape, scratch=(), flops=2_000_000, name=None, **specs):
    return pl.pallas_call(
        kernel,
        **specs,
        out_shape=out_shape,
        scratch_shapes=scratch,
        compiler_params=pltpu.CompilerParams(vmem_limit_bytes=8 << 20),
        cost_estimate=pl.CostEstimate(flops=flops, bytes_accessed=200_000, transcendentals=0),
        name=name,
    )


def solution(mesh):
    parts, majors, subs, inners = (mesh.shape[name] for name in ("parts", "tm", "sub", "inner"))
    axes = ("tm", "sub", "inner")
    low = 2 if majors % 2 == 0 else 1
    blocks = majors // low
    group = low * subs

    def flat(block, place, inner):
        return (block * group + place) * inners + inner

    def partner(place, turn, count):
        return place ^ turn if count & (count - 1) == 0 else (place + turn) % count

    def origin(place, turn, count):
        return place ^ turn if count & (count - 1) == 0 else lax.rem(place - turn + count, count)

    def inner_place():
        return lax.axis_index("inner")

    def group_place():
        return lax.rem(lax.axis_index("tm"), low) * subs + lax.axis_index("sub")

    def shards(guess, start, layer_weight, layer_bias, amplitude):
        rows, size = guess.shape
        width, hidden = size // 2, layer_weight.shape[0]
        f32 = functools.partial(jax.ShapeDtypeStruct, dtype=jnp.float32)
        packed = f32((size + 8, size))
        weight_t = layer_weight.T
        nodes = rows // 2 - 1
        total, first, tree, kicks, kick_first, shifts, curve, guess, weight_t = call(
            local_kernel,
            [packed, f32((8, size)), f32((nodes, size + PAD, size)), f32((rows // 2, width, size)),
             f32((width, size)), f32((rows, size)), f32((rows, hidden)), f32((rows, size)), f32((width, hidden))],
            [pltpu.VMEM((1, size), jnp.float32), pltpu.VMEM((1, hidden), jnp.float32), pltpu.VMEM((1, hidden), jnp.float32),
             pltpu.VMEM(((rows + 1) * width, hidden), jnp.bfloat16), pltpu.VMEM(((rows + 1) * width, hidden), jnp.bfloat16),
             pltpu.SemaphoreType.DMA((5,))],
            name="local_maps", flops=100_000_000, in_specs=[pl.BlockSpec(memory_space=pltpu.HBM)] * 5,
        )(*(pltpu.with_memory_space_constraint(value, pltpu.HBM) for value in (
            guess, start[None, :], weight_t, layer_bias[None, :], amplitude[None, :])))

        def exchange(value, pairs):
            return lax.ppermute(value, axes, pairs)

        inner_maps = [total]
        for turn in range(1, inners):
            inner_maps.append(exchange(total, [
                (flat(b, g, i), flat(b, g, partner(i, turn, inners)))
                for b in range(blocks) for g in range(group) for i in range(inners)]))
        inner_source = functools.partial(origin, count=inners)
        chip = total
        if inners > 1:
            chip = call(functools.partial(total_kernel, inner_source, inner_place, inners), packed,
                        [pltpu.VMEM((inners,) + packed.shape, jnp.float32)], name="chip_total")(*inner_maps)
        group_maps = [chip]
        for turn in range(1, group):
            group_maps.append(exchange(chip, [
                (flat(b, g, i), flat(b, partner(g, turn, group), (i + 1) % inners))
                for b in range(blocks) for g in range(group) for i in range(inners)]))
        group_source = functools.partial(origin, count=group)
        group_stack = [pltpu.VMEM((group,) + packed.shape, jnp.float32)]

        entering = first
        ahead = []
        held = lax.optimization_barrier((tree, kicks, chip))[:2]
        local, offsets = call(
            prefix_kernel, [f32((rows, size, size)), f32((rows, size))],
            [pltpu.VMEM(((rows - 1) * width, hidden), jnp.bfloat16)] * 2, name="local_prefix", flops=20_000_000_000,
        )(*held, kick_first, shifts, curve, guess, weight_t)
        if blocks > 1:
            block = lax.axis_index("tm") // low
            top = 1
            while top * 2 < blocks:
                top *= 2
            if blocks > 2:
                span = call(functools.partial(total_kernel, group_source, group_place, group), packed, group_stack,
                            name="block_total")(*group_maps)
            reach = None
            turn = 1
            while turn < top:
                arrived = exchange(span, [
                    (flat(b, g, i), flat((b ^ turn) % blocks if (b ^ turn) < blocks else b, g, (i + 1) % inners))
                    for b in range(blocks) for g in range(group) for i in range(inners)])
                upper = (block & turn) != 0
                known = (block ^ turn) < blocks
                early, late = jnp.where(upper, arrived, span), jnp.where(upper, span, arrived)
                joined = call(lambda a_ref, b_ref, o_ref: o_ref.__setitem__(..., compose(a_ref[...], b_ref[...])),
                              packed, name="span_total")(early, late)
                ahead.append((upper, arrived))
                span = jnp.where(known | upper, joined, span)
                turn *= 2
            if blocks == 2:
                reach = call(functools.partial(reach_kernel, group_source, group_place, group), f32((8, size)),
                             group_stack, name="block_reach")(first, *group_maps)
            else:
                reach = call(lambda f_ref, m_ref, o_ref: o_ref.__setitem__(..., apply(f_ref[...], m_ref[...])),
                             f32((8, size)), name="span_reach")(first, span)
            if blocks == 2 * top:
                pairs = [(flat(b, g, i), flat(b ^ top, g, (i + 1) % inners))
                         for b in range(blocks) for g in range(group) for i in range(inners)]
            else:
                pairs = [(flat(b, g, i), flat((b + top) % blocks, g, (i + 1) % inners))
                         for b in range(blocks) for g in range(group) for i in range(inners)]
            arrived = exchange(reach, pairs)
            if blocks == 2:
                entering = arrived
            else:
                entering = jnp.where(block >= top, arrived, first)
            for upper, value in reversed(ahead):
                moved = call(lambda f_ref, m_ref, o_ref: o_ref.__setitem__(..., apply(f_ref[...], m_ref[...])),
                             f32((8, size)), name="span_step")(entering, value)
                entering = jnp.where(upper, moved, entering)

        groups = []
        maps = []
        scratch = []
        if group > 1:
            groups.append((group_source, group_place, group))
            maps += group_maps
            scratch += group_stack
        if inners > 1:
            groups.append((inner_source, inner_place, inners))
            maps += inner_maps
            scratch.append(pltpu.VMEM((inners,) + packed.shape, jnp.float32))
        scale, shift, base = call(
            functools.partial(ahead_kernel, groups), [f32((size, size)), f32((size, size)), f32((8, size))], scratch,
            name="block_prefix", flops=2_000_000_000)(guess, *maps)

        def later_block():
            return lax.axis_index("tm") >= low if blocks == 2 else blocks > 2

        return call(functools.partial(finish_kernel, later_block), f32((rows, size)), name="finish")(
            entering, first, scale, shift, base, local, offsets)

    placed = (P(("parts",) + axes, None), P("parts"), P(), P(), P())
    return jax.shard_map(
        shards,
        mesh=mesh,
        in_specs=placed,
        out_specs=P(("parts",) + axes, None),
        check_vma=False,
    )
```

```python
import functools
import jax
import jax.numpy as jnp
from jax import lax
from jax.experimental import pallas as pl
from jax.experimental.pallas import tpu as pltpu
from jax.sharding import PartitionSpec as P

step_size = 0.04
curvature = 0.5
PAD = 16

NN = (((1,), (0,)), ((), ()))
NT = (((1,), (1,)), ((), ()))


def split(value):
    high = value.astype(jnp.bfloat16)
    return high, (value - high.astype(jnp.float32)).astype(jnp.bfloat16)


def dot3(left, right, dims=NN):
    (left_high, left_low), (right_high, right_low) = left, right
    one = functools.partial(lax.dot_general, dimension_numbers=dims, preferred_element_type=jnp.float32)
    return one(left_high, right_high) + (one(left_high, right_low) + one(left_low, right_high))


def dot3w(left, right):
    (left_high, left_low), (right_high, right_low) = left, right
    size = right_high.shape[1]
    both = jnp.dot(left_high, jnp.concatenate([right_high, right_low], axis=1), preferred_element_type=jnp.float32)
    return both[:, :size] + (both[:, size:] + jnp.dot(left_low, right_high, preferred_element_type=jnp.float32))


def join(early, late):
    state = late.shape[1]
    product = dot3w(split(early), split(late[:state]))
    return jnp.concatenate([product[:state], product[state:] + late[state:]], axis=0)


def local_kernel(guess_in, start_in, weight_in, bias_in, amp_in,
                 total_ref, first_ref, tree_ref, kicks_ref, kick_first_ref, shifts_ref, curve_ref, guess_ref, weight_ref,
                 start_ref, bias_ref, amp_ref, high_ref, low_ref, arrived):
    copies = [
        pltpu.make_async_copy(source, target, arrived.at[index])
        for index, (source, target) in enumerate((
            (weight_in, weight_ref), (guess_in, guess_ref), (start_in, start_ref),
            (bias_in, bias_ref), (amp_in, amp_ref)))
    ]
    for copy in copies:
        copy.start()
    for copy in copies:
        copy.wait()
    rows, state = guess_ref.shape
    width = state // 2
    h = step_size
    guess = guess_ref[...]
    hidden = weight_ref.shape[1]
    points = jnp.concatenate([guess, jnp.broadcast_to(start_ref[...], (8, state))], axis=0)
    weight = weight_ref[...]
    weight_high, weight_low = split(weight)
    wide = jnp.concatenate([weight_high, weight_high, weight_low, jnp.zeros_like(weight_low)], axis=0)
    double_high = jnp.concatenate([weight_high, weight_high], axis=0)
    double = jnp.concatenate([double_high, weight_low, weight_low], axis=0)
    bias, amp = bias_ref[...], amp_ref[...]

    def side(value):
        return lax.broadcasted_iota(jnp.int32, value.shape, 1) >= width

    def swap(value):
        return jnp.concatenate([value[:, width:], value[:, :width]], axis=1)

    def stack_left(twice):
        high, low = split(twice)
        mixed = jnp.where(side(twice), twice - high.astype(jnp.float32), high.astype(jnp.float32))
        return jnp.concatenate([mixed.astype(jnp.bfloat16), high], axis=1)

    def stack_right(value):
        high, low = split(value)
        return jnp.concatenate([high, high, low, jnp.zeros_like(low)], axis=0)

    def to_hidden(twice):
        return jnp.dot(stack_left(twice), wide, preferred_element_type=jnp.float32)

    def from_hidden(value):
        high, low = split(value)
        both = lax.dot_general(high, double, NT, preferred_element_type=jnp.float32)
        small = lax.dot_general(low, double_high, NT, preferred_element_type=jnp.float32)
        return both[:, :state] + (both[:, state:] + small)

    swapped = swap(points)
    right = side(points)
    coords = jnp.where(right, swapped, points)
    momenta = jnp.where(right, points, swapped)
    gate = jax.nn.sigmoid(to_hidden(coords) + bias)
    scaled = amp * gate
    curve_zero = scaled * (1.0 - gate)
    half = momenta - 0.5 * h * (from_hidden(scaled) + curvature * coords)
    moved = coords + h * half

    pushed = moved[:rows] - jnp.concatenate([coords[1:rows], coords[:1]], axis=0)
    curve_next = jnp.concatenate([curve_zero[1:rows], jnp.zeros((1, hidden), jnp.float32)], axis=0)
    spread_out = to_hidden(jnp.concatenate([moved, pushed], axis=0))
    count = points.shape[0]
    gate = jax.nn.sigmoid(spread_out[:count] + bias)
    scaled = amp * gate
    curve_one = scaled * (1.0 - gate)
    gathered = from_hidden(jnp.concatenate([scaled, spread_out[count:] * curve_next], axis=0))
    landed = half - 0.5 * h * (gathered[:count] + curvature * moved)
    image = jnp.where(right, landed, moved)
    first_ref[...] = image[rows:]
    kicked = 0.5 * h * (gathered[count:] + curvature * pushed)
    residual = image[:rows] - jnp.concatenate([guess[1:], guess[:1]], axis=0)
    shifts = residual - jnp.where(right[:rows], kicked, 0.0)
    row_id = lax.broadcasted_iota(jnp.int32, (rows, state), 0)
    shifts = jnp.where(row_id == rows - 1, image[:rows], shifts)
    shifts_ref[...] = shifts
    curve_ref[...] = curve_zero[:rows]
    drifted = shifts + jnp.where(right[:rows], 0.0, h * swap(shifts))

    line = lax.broadcasted_iota(jnp.int32, (width, state), 0)
    lane = lax.broadcasted_iota(jnp.int32, (width, state), 1)
    unit2 = jnp.where((lane == line) | (lane == line + width), 1.0, 0.0)
    right = lane >= width
    unit_top = jnp.where(lane == line, 1.0, 0.0)
    unit_low = jnp.where(lane == line + width, 1.0, 0.0)
    between = (curve_one[:rows] + curve_next) * (0.5 * h)
    rows_of_kick = [curve_zero[0:1] * (0.5 * h)] + [between[j:j + 1] for j in range(rows)]
    for j, weights_row in enumerate(rows_of_kick):
        scaled_high, scaled_low = split(weight * weights_row)
        high_ref[j * width:(j + 1) * width] = scaled_high
        low_ref[j * width:(j + 1) * width] = scaled_low
    product = lax.dot_general(high_ref[...], double, NT, preferred_element_type=jnp.float32)
    small = lax.dot_general(low_ref[...], double_high, NT, preferred_element_type=jnp.float32)
    product = product[:, :state] + (product[:, state:] + small)
    kicks = [
        product[j * width:(j + 1) * width] + (0.5 * h * curvature * (1 if j in (0, rows) else 2)) * unit2
        for j in range(rows + 1)
    ]
    kick_first, kicks = kicks[0], kicks[1:]
    kick_first_ref[...] = kick_first
    for j in range(0, rows, 2):
        kicks_ref[j // 2] = kicks[j]

    level = []
    drifted_twice = jnp.where(side(drifted), swap(drifted), drifted)
    for k in range(rows // 2):
        a, b = kicks[2 * k], kicks[2 * k + 1]
        moved_row = jnp.broadcast_to(drifted_twice[2 * k:2 * k + 1], (PAD, state))
        both = jnp.dot(stack_left(jnp.concatenate([a, moved_row], axis=0)), stack_right(b), preferred_element_type=jnp.float32)
        prod = both[:width]
        top = unit_top - jnp.where(right, a + b - h * prod, h * a)
        low = 2 * h * unit_top + unit_low - jnp.where(right, h * a + 2 * h * b - (h * h) * prod, (h * h) * a)
        if k == 0:
            top = top - jnp.dot(stack_left(kick_first), stack_right(low), preferred_element_type=jnp.float32)
        tail = drifted[2 * k:2 * k + 1] - jnp.where(right[:PAD], both[width:], 0.0) + shifts[2 * k + 1:2 * k + 2]
        level.append(jnp.concatenate([top, low, tail], axis=0))
    slot = 0
    while len(level) > 1:
        for item in level[::2]:
            tree_ref[slot] = item
            slot += 1
        level = [join(level[i], level[i + 1]) for i in range(0, len(level), 2)]
    total = level[0]
    total_ref[:state] = total[:state]
    tail_row = lax.broadcasted_iota(jnp.int32, (8, state), 0)
    total_ref[state:] = jnp.where(tail_row == 0, total[state:state + 8], jnp.broadcast_to(guess[0:1], (8, state)))


def spread(packed, state):
    return packed[:state], packed[state:state + 1], packed[state + 1:state + 2]


def apply(state_rows, packed):
    size = packed.shape[1]
    matrix, shift, origin = spread(packed, size)
    return dot3(split(state_rows - origin), split(matrix)) + shift


def compose(early, late):
    size = early.shape[1]
    matrix_a, shift_a, origin_a = spread(early, size)
    matrix_b, shift_b, origin_b = spread(late, size)
    left = jnp.concatenate([matrix_a, jnp.broadcast_to(shift_a - origin_b, (PAD, size))], axis=0)
    product = dot3(split(left), split(matrix_b))
    tail_row = lax.broadcasted_iota(jnp.int32, (8, size), 0)
    tail = jnp.where(tail_row == 0, product[size:size + 8] + shift_b, jnp.broadcast_to(origin_a, (8, size)))
    return jnp.concatenate([product[:size], tail], axis=0)


def ordered(own_ref, others, stack_ref, place, source):
    stack_ref[place] = own_ref[...]
    for index, other in enumerate(others):
        stack_ref[source(place, index + 1)] = other[...]


def total_kernel(source, axis_place, count, own_ref, *refs):
    others, (out_ref, stack_ref) = refs[:count - 1], refs[count - 1:]
    ordered(own_ref, others, stack_ref, axis_place(), source)
    total = stack_ref[0]
    for position in range(1, count):
        total = compose(total, stack_ref[position])
    out_ref[...] = total


def reach_kernel(source, axis_place, count, first_ref, own_ref, *refs):
    others, (out_ref, stack_ref) = refs[:count - 1], refs[count - 1:]
    ordered(own_ref, others, stack_ref, axis_place(), source)
    size = first_ref.shape[1]
    state = first_ref[0:1]
    for position in range(0, count - 1, 2):
        matrix_a, shift_a, origin_a = spread(stack_ref[position], size)
        matrix_b, shift_b, origin_b = spread(stack_ref[position + 1], size)
        turned = jnp.sum(matrix_a.T * (state - origin_a), axis=1, keepdims=True)
        column = jnp.broadcast_to(shift_a - origin_b, (size, size)).T
        state = jnp.sum(matrix_b * turned, axis=0, keepdims=True) + (
            jnp.sum(matrix_b * column, axis=0, keepdims=True) + shift_b)
    state = jnp.broadcast_to(state, (8, size))
    if count % 2:
        state = apply(state, stack_ref[count - 1])
    out_ref[...] = state


def prefix_kernel(tree_ref, kicks_ref, kick_first_ref, shifts_ref, curve_ref, guess_ref, weight_ref,
                  maps_ref, offsets_ref, high_ref, low_ref):
    rows, size = guess_ref.shape
    width = size // 2
    h = step_size
    weight = weight_ref[...]
    double2 = split(jnp.concatenate([weight, weight], axis=0))
    for j in range(1, rows):
        scaled_high, scaled_low = split(weight * (curve_ref[j:j + 1] * (0.5 * h)))
        high_ref[(j - 1) * width:j * width] = scaled_high
        low_ref[(j - 1) * width:j * width] = scaled_low
    product = lax.dot_general(high_ref[...], jnp.concatenate(double2, axis=0), NT, preferred_element_type=jnp.float32)
    small = lax.dot_general(low_ref[...], double2[0], NT, preferred_element_type=jnp.float32)
    product = product[:, :size] + (product[:, size:] + small)
    line = lax.broadcasted_iota(jnp.int32, (width, size), 0)
    lane = lax.broadcasted_iota(jnp.int32, (width, size), 1)
    unit2 = jnp.where((lane == line) | (lane == line + width), 0.5 * h * curvature, 0.0)
    whole_line = lax.broadcasted_iota(jnp.int32, (size + PAD, size), 0)
    whole_lane = lax.broadcasted_iota(jnp.int32, (size + PAD, size), 1)
    left = whole_lane < width
    unit = jnp.where(whole_line == whole_lane, 1.0, 0.0)

    def kick(item, matrix):
        return item - jnp.where(left, 0.0, dot3w(split(item[:, :width]), split(matrix)))

    def drift(item):
        other = jnp.concatenate([item[:, width:], item[:, :width]], axis=1)
        return item + jnp.where(left, h * other, 0.0)

    count = rows // 2
    starts, sizes, n = [0], [], count
    while n > 1:
        sizes.append(n // 2)
        starts.append(starts[-1] + n // 2)
        n //= 2
    kicked = {0: kick(unit, kick_first_ref[...])}
    for k in range(1, count):
        low = k & -k
        node = tree_ref[starts[low.bit_length() - 1] + (k - low) // low // 2]
        kicked[2 * k] = node if k == low else join(kicked[2 * (k - low)], node)
    maps_ref[0] = unit[:size]
    offsets_ref[0:1] = guess_ref[0:1]
    for k in range(count):
        after = kick(drift(kicked[2 * k]), kicks_ref[k])
        tail = after[size:] + shifts_ref[2 * k:2 * k + 1]
        kicked[2 * k + 1] = jnp.concatenate([after[:size], tail], axis=0)
    for t in range(1, rows):
        item = kick(kicked[t], -(product[(t - 1) * width:t * width] + unit2))
        maps_ref[t] = item[:size]
        offsets_ref[t:t + 1] = item[size:size + 1] + guess_ref[t:t + 1]


def ahead_kernel(groups, guess_ref, *refs):
    size = guess_ref.shape[1]
    out_ref, shift_ref, origin_ref = refs[-3 - len(groups):len(refs) - len(groups)]
    stacks = refs[len(refs) - len(groups):]
    line = lax.broadcasted_iota(jnp.int32, (size + 8, size), 0)
    lane = lax.broadcasted_iota(jnp.int32, (size + 8, size), 1)
    total = jnp.where(line == lane, 1.0, 0.0)
    empty = True
    used = 0
    for (source, axis_place, count), stack_ref in zip(groups, stacks):
        own_ref, others = refs[used], refs[used + 1:used + count]
        used += count
        place = axis_place()
        ordered(own_ref, others, stack_ref, place, source)

        def body(i, carry, stack_ref=stack_ref):
            return compose(carry, stack_ref[i])

        if empty is True:
            total = lax.fori_loop(1, place, body, jnp.where(place > 0, stack_ref[0], total))
            empty = place == 0
        else:
            first = jnp.where(empty, stack_ref[0], compose(total, stack_ref[0]))
            total = lax.fori_loop(1, place, body, jnp.where(place > 0, first, total))
            empty = empty & (place == 0)
    out_ref[...] = total[:size].T
    shift = total[size:size + 1] - guess_ref[0:1]
    shift_ref[...] = jnp.broadcast_to(shift, (size, size)).T
    origin_ref[...] = jnp.broadcast_to(total[size + 1:size + 2], (8, size))


def finish_kernel(later_block, arrived_ref, first_ref, ahead_ref, shift_ref, origin_ref, maps_ref, offsets_ref, out_ref):
    rows, size = offsets_ref.shape
    state = jnp.where(later_block(), arrived_ref[0:1], first_ref[0:1]) - origin_ref[0:1]
    delta = jnp.sum(ahead_ref[...] * state, axis=1, keepdims=True) + shift_ref[...]
    pieces = [jnp.sum(maps_ref[t] * delta, axis=0, keepdims=True) for t in range(rows)]
    out_ref[...] = jnp.concatenate(pieces, axis=0) + offsets_ref[...]


def call(kernel, out_shape, scratch=(), flops=2_000_000, name=None, **specs):
    return pl.pallas_call(
        kernel,
        **specs,
        out_shape=out_shape,
        scratch_shapes=scratch,
        compiler_params=pltpu.CompilerParams(vmem_limit_bytes=8 << 20),
        cost_estimate=pl.CostEstimate(flops=flops, bytes_accessed=200_000, transcendentals=0),
        name=name,
    )


def solution(mesh):
    parts, majors, subs, inners = (mesh.shape[name] for name in ("parts", "tm", "sub", "inner"))
    axes = ("tm", "sub", "inner")
    low = 2 if majors % 2 == 0 else 1
    blocks = majors // low
    group = low * subs

    def flat(block, place, inner):
        return (block * group + place) * inners + inner

    def partner(place, turn, count):
        return place ^ turn if count & (count - 1) == 0 else (place + turn) % count

    def origin(place, turn, count):
        return place ^ turn if count & (count - 1) == 0 else lax.rem(place - turn + count, count)

    def inner_place():
        return lax.axis_index("inner")

    def group_place():
        return lax.rem(lax.axis_index("tm"), low) * subs + lax.axis_index("sub")

    def shards(guess, start, layer_weight, layer_bias, amplitude):
        rows, size = guess.shape
        width, hidden = size // 2, layer_weight.shape[0]
        f32 = functools.partial(jax.ShapeDtypeStruct, dtype=jnp.float32)
        packed = f32((size + 8, size))
        weight_t = layer_weight.T
        nodes = rows // 2 - 1
        total, first, tree, kicks, kick_first, shifts, curve, guess, weight_t = call(
            local_kernel,
            [packed, f32((8, size)), f32((nodes, size + PAD, size)), f32((rows // 2, width, size)),
             f32((width, size)), f32((rows, size)), f32((rows, hidden)), f32((rows, size)), f32((width, hidden))],
            [pltpu.VMEM((1, size), jnp.float32), pltpu.VMEM((1, hidden), jnp.float32), pltpu.VMEM((1, hidden), jnp.float32),
             pltpu.VMEM(((rows + 1) * width, hidden), jnp.bfloat16), pltpu.VMEM(((rows + 1) * width, hidden), jnp.bfloat16),
             pltpu.SemaphoreType.DMA((5,))],
            name="local_maps", flops=100_000_000, in_specs=[pl.BlockSpec(memory_space=pltpu.HBM)] * 5,
        )(*(pltpu.with_memory_space_constraint(value, pltpu.HBM) for value in (
            guess, start[None, :], weight_t, layer_bias[None, :], amplitude[None, :])))

        def exchange(value, pairs):
            return lax.ppermute(value, axes, pairs)

        inner_maps = [total]
        for turn in range(1, inners):
            inner_maps.append(exchange(total, [
                (flat(b, g, i), flat(b, g, partner(i, turn, inners)))
                for b in range(blocks) for g in range(group) for i in range(inners)]))
        inner_source = functools.partial(origin, count=inners)
        chip = total
        if inners > 1:
            chip = call(functools.partial(total_kernel, inner_source, inner_place, inners), packed,
                        [pltpu.VMEM((inners,) + packed.shape, jnp.float32)], name="chip_total")(*inner_maps)
        group_maps = [chip]
        for turn in range(1, group):
            group_maps.append(exchange(chip, [
                (flat(b, g, i), flat(b, partner(g, turn, group), (i + 1) % inners))
                for b in range(blocks) for g in range(group) for i in range(inners)]))
        group_source = functools.partial(origin, count=group)
        group_stack = [pltpu.VMEM((group,) + packed.shape, jnp.float32)]

        entering = first
        ahead = []
        held = lax.optimization_barrier((tree, kicks, chip))[:2]
        local, offsets = call(
            prefix_kernel, [f32((rows, size, size)), f32((rows, size))],
            [pltpu.VMEM(((rows - 1) * width, hidden), jnp.bfloat16)] * 2, name="local_prefix", flops=20_000_000_000,
        )(*held, kick_first, shifts, curve, guess, weight_t)
        if blocks > 1:
            block = lax.axis_index("tm") // low
            top = 1
            while top * 2 < blocks:
                top *= 2
            if blocks > 2:
                span = call(functools.partial(total_kernel, group_source, group_place, group), packed, group_stack,
                            name="block_total")(*group_maps)
            reach = None
            turn = 1
            while turn < top:
                arrived = exchange(span, [
                    (flat(b, g, i), flat((b ^ turn) % blocks if (b ^ turn) < blocks else b, g, (i + 1) % inners))
                    for b in range(blocks) for g in range(group) for i in range(inners)])
                upper = (block & turn) != 0
                known = (block ^ turn) < blocks
                early, late = jnp.where(upper, arrived, span), jnp.where(upper, span, arrived)
                joined = call(lambda a_ref, b_ref, o_ref: o_ref.__setitem__(..., compose(a_ref[...], b_ref[...])),
                              packed, name="span_total")(early, late)
                ahead.append((upper, arrived))
                span = jnp.where(known | upper, joined, span)
                turn *= 2
            if blocks == 2:
                reach = call(functools.partial(reach_kernel, group_source, group_place, group), f32((8, size)),
                             group_stack, name="block_reach")(first, *group_maps)
            else:
                reach = call(lambda f_ref, m_ref, o_ref: o_ref.__setitem__(..., apply(f_ref[...], m_ref[...])),
                             f32((8, size)), name="span_reach")(first, span)
            if blocks == 2 * top:
                pairs = [(flat(b, g, i), flat(b ^ top, g, (i + 1) % inners))
                         for b in range(blocks) for g in range(group) for i in range(inners)]
            else:
                pairs = [(flat(b, g, i), flat((b + top) % blocks, g, (i + 1) % inners))
                         for b in range(blocks) for g in range(group) for i in range(inners)]
            arrived = exchange(reach, pairs)
            if blocks == 2:
                entering = arrived
            else:
                entering = jnp.where(block >= top, arrived, first)
            for upper, value in reversed(ahead):
                moved = call(lambda f_ref, m_ref, o_ref: o_ref.__setitem__(..., apply(f_ref[...], m_ref[...])),
                             f32((8, size)), name="span_step")(entering, value)
                entering = jnp.where(upper, moved, entering)

        groups = []
        maps = []
        scratch = []
        if group > 1:
            groups.append((group_source, group_place, group))
            maps += group_maps
            scratch += group_stack
        if inners > 1:
            groups.append((inner_source, inner_place, inners))
            maps += inner_maps
            scratch.append(pltpu.VMEM((inners,) + packed.shape, jnp.float32))
        scale, shift, base = call(
            functools.partial(ahead_kernel, groups), [f32((size, size)), f32((size, size)), f32((8, size))], scratch,
            name="block_prefix", flops=2_000_000_000)(guess, *maps)

        def later_block():
            return lax.axis_index("tm") >= low if blocks == 2 else blocks > 2

        return call(functools.partial(finish_kernel, later_block), f32((rows, size)), name="finish")(
            entering, first, scale, shift, base, local, offsets)

    placed = (P(("parts",) + axes, None), P("parts"), P(), P(), P())
    return jax.shard_map(
        shards,
        mesh=mesh,
        in_specs=placed,
        out_specs=P(("parts",) + axes, None),
        check_vma=False,
    )
```
